64 devices in a mesh: dp: 8 (over x, y, core), tp: 8 (over z).
Axes of the slice: x: 2, y: 2, z: 8, core: 2. Of those that a mesh axis runs over, the one named last changes fastest.
The devices are a block of a 4x4x8 slice.
Arguments:
- x: bfloat16 [18432, 3840], P(('dp', 'tp')), parts along dimension 0
- w_gate: bfloat16 [3840, 15360], P(None, 'tp')
- w_up: bfloat16 [3840, 15360], P(None, 'tp')
- w_down: bfloat16 [15360, 3840], P('tp')
Outputs:
- output: bfloat16 [18432, 3840], P(('dp', 'tp')), parts along dimension 0
There are 8 independent parts. The reference program is written for one: setup_inputs(seed, part) draws one part's arguments, and reference() takes and returns one part's arrays. A program takes and returns all parts, laid end to end along the dimension named above; an argument that names none is the same for every part.
All inputs are finite; a program needn't handle non-finite values.
Results may differ from the reference program's by a relative error of at most 0.016.
Values are sent between devices in bfloat16 or wider.
A program may use at most 768 MiB of HBM per device.

```python
import jax
import jax.numpy as jnp

ROWS = 2304
D = 3840
FF = 15360


def setup_inputs(seed: int = 0, part: int = 0) -> dict:
    kx, kg, ku, kd = jax.random.split(jax.random.key(seed), 4)
    drawn = {
        "x": jax.random.normal(jax.random.fold_in(kx, part), (ROWS, D), jnp.float32),
        "w_gate": jax.random.normal(kg, (D, FF), jnp.float32) * D**-0.5,
        "w_up": jax.random.normal(ku, (D, FF), jnp.float32) * D**-0.5,
        "w_down": jax.random.normal(kd, (FF, D), jnp.float32) * FF**-0.5,
    }
    return {k: v.astype(jnp.bfloat16) for k, v in drawn.items()}


def reference(x, w_gate, w_up, w_down):
    gate = jnp.dot(x, w_gate, preferred_element_type=jnp.float32)
    up = jnp.dot(x, w_up, preferred_element_type=jnp.float32)
    hidden = (jax.nn.gelu(gate) * up).astype(jnp.bfloat16)
    return jnp.dot(hidden, w_down, preferred_element_type=jnp.float32).astype(jnp.bfloat16)
```

```python
import functools

import jax
import jax.numpy as jnp
from jax import lax
from jax.experimental import pallas as pl
from jax.experimental.pallas import tpu as pltpu
from jax.sharding import PartitionSpec as P

MESH = pl.DeviceIdType.MESH
F32 = jnp.float32
BF16 = jnp.bfloat16
CHUNKS = 3
TILE = 256
PAIR = (5, 7, 3, 6, 1, 4, 2)
LONG = (False, True, False, True, False, True, True)
FROM = (None, None, 0, 1, 2, 3, 5)


def kernel(n, x, wg, wu, wd, y, gx, wgv, wuv, wdv, hid, xv, stage, first, total,
           w_sem, x_sem, ag_send, ag_recv, rs_send, rs_recv, free):
    me = lax.axis_index("tp")
    right, left = {"tp": lax.rem(me + 1, n)}, {"tp": lax.rem(me + n - 1, n)}
    half = x.shape[0] // 2
    depth, width = wgv.shape
    cols = x.shape[1] // CHUNKS

    wcopies = [pltpu.make_async_copy(a, b, w_sem.at[i]) for i, (a, b) in enumerate(((wg, wgv), (wu, wuv), (wd, wdv)))]

    barrier = pltpu.get_barrier_semaphore()
    for neighbour in (left, right):
        pl.semaphore_signal(barrier, inc=1, device_id=neighbour, device_id_type=MESH)
    pl.semaphore_wait(barrier, 2)

    def ag(k, d, own=False):
        at = pl.multiple_of(lax.rem(k + 1 + d, 2) * half, half)
        src = x.at[pl.ds(at, half)] if own else gx.at[lax.rem(k + n - 4, n - 1), pl.ds(at, half)]
        return pltpu.make_async_remote_copy(
            src_ref=src, dst_ref=gx.at[k - 1, pl.ds(at, half)], send_sem=ag_send.at[d, k - 1], recv_sem=ag_recv.at[d, k - 1],
            device_id=(right, left)[d], device_id_type=MESH)

    for k in (1, 2):
        for d in (0, 1):
            ag(jnp.int32(k), d, own=True).start()
    for c in wcopies:
        c.start()

    def hidden_of(k):
        def tile(at, size):
            gate = jnp.dot(xv[...], wgv[:, pl.ds(at, size)], preferred_element_type=F32)
            up = jnp.dot(xv[...], wuv[:, pl.ds(at, size)], preferred_element_type=F32)
            hid[k, :, pl.ds(at, size)] = (jax.nn.gelu(gate) * up).astype(BF16)

        @pl.loop(0, width // TILE)
        def _(t):
            tile(pl.multiple_of(t * TILE, TILE), TILE)

        if width % TILE:
            tile(width - width % TILE, width % TILE)

    def gather_step(k):
        for d in (0, 1):
            ag(k, d).wait_recv()

        @pl.when(k <= 5)
        def _():
            for d in (0, 1):
                ag(k + 2, d).start()

        load = pltpu.make_async_copy(gx.at[k - 1], xv, x_sem)
        load.start()
        load.wait()
        hidden_of(k)

    def rs(j, c, h):
        if j == 0:
            dst = first.at[h, c]
        else:
            at = pl.multiple_of(((j - 1) * CHUNKS + c) * half, half)
            dst = (wgv, wuv)[h].at[pl.ds(at, half), pl.ds(0, cols)]
        to_right = (h == 0) == LONG[j]
        return pltpu.make_async_remote_copy(
            src_ref=stage.at[j % 2, c, pl.ds(h * half, half)], dst_ref=dst,
            send_sem=rs_send.at[h, j, c], recv_sem=rs_recv.at[h, j, c],
            device_id=right if to_right else left, device_id_type=MESH)

    def landed(j, c, h, at):
        if j == 0:
            return first[h, c, :, pl.ds(at, TILE)].astype(F32)
        row = pl.multiple_of(((j - 1) * CHUNKS + c) * half, half)
        return (wgv, wuv)[h][pl.ds(row, half), pl.ds(at, TILE)].astype(F32)

    def term(k, c, at):
        return jnp.dot(hid[k], wdv[:, pl.ds(pl.multiple_of(c * cols + at, TILE), TILE)], preferred_element_type=F32)

    def sum_step(j):
        @pl.loop(0, CHUNKS)
        def _(c):
            if FROM[j] is not None:
                for h in (0, 1):
                    rs(FROM[j], c, h).wait_recv()
            if j >= 2:
                for h in (0, 1):
                    rs(j - 2, c, h).wait_send()

            @pl.loop(0, cols // TILE)
            def _(t):
                at = pl.multiple_of(t * TILE, TILE)
                acc = term(PAIR[j], c, at)
                for h in (0, 1):
                    part = acc[h * half:(h + 1) * half]
                    if FROM[j] is not None:
                        part = part + landed(FROM[j], c, h, at)
                    stage[j % 2, c, pl.ds(h * half, half), pl.ds(at, TILE)] = part.astype(BF16)

            for h in (0, 1):
                rs(j, c, h).start()

    own = pltpu.make_async_copy(x, xv, x_sem)
    own.start()
    own.wait()
    wcopies[0].wait()
    wcopies[1].wait()
    hidden_of(0)
    pl.loop(1, 6)(gather_step)
    wcopies[2].wait()
    sum_step(0)
    pl.loop(6, 8)(gather_step)
    pl.semaphore_signal(free.at[1], inc=1, device_id=right, device_id_type=MESH)
    pl.semaphore_signal(free.at[0], inc=1, device_id=left, device_id_type=MESH)
    pl.semaphore_wait(free.at[0], 1)
    pl.semaphore_wait(free.at[1], 1)
    for j in range(1, 7):
        sum_step(j)

    @pl.loop(0, CHUNKS)
    def _(c):
        for h in (0, 1):
            rs(4, c, h).wait_recv()

        @pl.loop(0, cols // TILE)
        def _(t):
            at = pl.multiple_of(t * TILE, TILE)
            acc = term(0, c, at)
            for h in (0, 1):
                total[pl.ds(h * half, half), pl.ds(at, TILE)] = acc[h * half:(h + 1) * half] + landed(4, c, h, at)

        for h in (0, 1):
            rs(6, c, h).wait_recv()

        @pl.loop(0, cols // TILE)
        def _(t):
            at = pl.multiple_of(t * TILE, TILE)
            for h in (0, 1):
                rows = pl.ds(h * half, half)
                y[rows, pl.ds(pl.multiple_of(c * cols + at, TILE), TILE)] = (
                    total[rows, pl.ds(at, TILE)] + landed(6, c, h, at)).astype(BF16)

    @pl.loop(0, CHUNKS)
    def _(c):
        for h in (0, 1):
            rs(5, c, h).wait_send()
            rs(6, c, h).wait_send()

    @pl.loop(1, 8)
    def _(k):
        for d in (0, 1):
            ag(k, d).wait_send()


def solution(mesh):
    n = mesh.shape["tp"]

    def step(x, w_gate, w_up, w_down):
        rows, d = x.shape
        width = w_gate.shape[1]
        half, cols = rows // 2, d // CHUNKS
        dma = pltpu.SemaphoreType.DMA
        y, _ = pl.pallas_call(
            functools.partial(kernel, n),
            out_shape=(pltpu.VMEM((rows, d), BF16), jax.ShapeDtypeStruct((n - 1, rows, d), BF16)),
            in_specs=[pl.BlockSpec(memory_space=pl.ANY)] * 4,
            out_specs=(pl.BlockSpec(memory_space=pltpu.VMEM), pl.BlockSpec(memory_space=pl.ANY)),
            scratch_shapes=[
                pltpu.VMEM((d, width), BF16),
                pltpu.VMEM((d, width), BF16),
                pltpu.VMEM((width, d), BF16),
                pltpu.VMEM((n, rows, width), BF16),
                pltpu.VMEM((rows, d), BF16),
                pltpu.VMEM((2, CHUNKS, rows, cols), BF16),
                pltpu.VMEM((2, CHUNKS, half, cols), BF16),
                pltpu.VMEM((rows, cols), F32),
                dma((3,)),
                dma,
                dma((2, n - 1)),
                dma((2, n - 1)),
                dma((2, 7, CHUNKS)),
                dma((2, 7, CHUNKS)),
                pltpu.SemaphoreType.REGULAR((2,)),
            ],
            compiler_params=pltpu.CompilerParams(
                collective_id=0, has_side_effects=True, vmem_limit_bytes=67043328 - 2 * rows * d),
            cost_estimate=pl.CostEstimate(
                flops=6 * n * rows * d * width, bytes_accessed=6 * d * width + 4 * n * rows * d, transcendentals=n * rows * width),
        )(x, w_gate, w_up, w_down)
        return y

    return jax.shard_map(
        step,
        mesh=mesh,
        in_specs=(P(("dp", "tp"), None), P(None, "tp"), P(None, "tp"), P("tp", None)),
        out_specs=P(("dp", "tp"), None),
        check_vma=False,
    )
```

```python
import functools

import jax
import jax.numpy as jnp
from jax import lax
from jax.experimental import pallas as pl
from jax.experimental.pallas import tpu as pltpu
from jax.sharding import PartitionSpec as P

MESH = pl.DeviceIdType.MESH
F32 = jnp.float32
BF16 = jnp.bfloat16
CHUNKS = 3
SHIFT = 16, 1024
TILE = 256
PAIR = (5, 7, 3, 6, 1, 4, 2)
LONG = (False, True, False, True, False, True, True)
FROM = (None, None, 0, 1, 2, 3, 5)


def kernel(n, x, wg, wu, wd, y, gx, wgv, wuv, wdv, hid, xv, stage, first, total,
           w_sem, x_sem, ag_send, ag_recv, last_send, last_recv, rs_send, rs_recv, free):
    me = lax.axis_index("tp")
    right, left = {"tp": lax.rem(me + 1, n)}, {"tp": lax.rem(me + n - 1, n)}
    half = x.shape[0] // 2
    depth, width = wgv.shape
    cols = x.shape[1] // CHUNKS

    wcopies = [pltpu.make_async_copy(a, b, w_sem.at[i]) for i, (a, b) in enumerate(((wg, wgv), (wu, wuv), (wd, wdv)))]

    barrier = pltpu.get_barrier_semaphore()
    for neighbour in (left, right):
        pl.semaphore_signal(barrier, inc=1, device_id=neighbour, device_id_type=MESH)
    pl.semaphore_wait(barrier, 2)

    def ag(k, d, own=False):
        at = pl.multiple_of(lax.rem(k + 1 + d, 2) * half, half)
        src = x.at[pl.ds(at, half)] if own else gx.at[lax.rem(k + n - 4, n - 1), pl.ds(at, half)]
        return pltpu.make_async_remote_copy(
            src_ref=src, dst_ref=gx.at[k - 1, pl.ds(at, half)], send_sem=ag_send.at[d, k - 1], recv_sem=ag_recv.at[d, k - 1],
            device_id=(right, left)[d], device_id_type=MESH)

    def last(i):
        r, c = SHIFT
        rows = pl.ds(0, half - r) if i == 0 else pl.ds(half - r, r)
        columns = (pl.ds(0, x.shape[1]), pl.ds(0, x.shape[1] - c), pl.ds(x.shape[1] - c, c))[i]
        return pltpu.make_async_remote_copy(
            src_ref=gx.at[n - 3 if i == 2 else n - 4, rows, columns], dst_ref=gx.at[n - 2, rows, columns],
            send_sem=last_send.at[i], recv_sem=last_recv.at[i], device_id=left if i == 2 else right, device_id_type=MESH)

    for k in (1, 2):
        for d in (0, 1):
            ag(jnp.int32(k), d, own=True).start()
    for c in wcopies:
        c.start()

    def hidden_of(k):
        def tile(at, size):
            gate = jnp.dot(xv[...], wgv[:, pl.ds(at, size)], preferred_element_type=F32)
            up = jnp.dot(xv[...], wuv[:, pl.ds(at, size)], preferred_element_type=F32)
            hid[k, :, pl.ds(at, size)] = (jax.nn.gelu(gate) * up).astype(BF16)

        @pl.loop(0, width // TILE)
        def _(t):
            tile(pl.multiple_of(t * TILE, TILE), TILE)

        if width % TILE:
            tile(width - width % TILE, width % TILE)

    def gather_step(k):
        for d in (0, 1):
            ag(k, d).wait_recv()

        @pl.when(k <= 4)
        def _():
            for d in (0, 1):
                ag(k + 2, d).start()

        @pl.when(k == 5)
        def _():
            last(0).start()
            last(1).start()
            ag(7, 1).start()

        @pl.when(k == 6)
        def _():
            last(2).start()

        load_hidden(k)

    def load_hidden(k):
        load = pltpu.make_async_copy(gx.at[k - 1], xv, x_sem)
        load.start()
        load.wait()
        hidden_of(k)

    def rs(j, c, h):
        if j == 0:
            dst = first.at[h, c]
        else:
            at = pl.multiple_of(((j - 1) * CHUNKS + c) * half, half)
            dst = (wgv, wuv)[h].at[pl.ds(at, half), pl.ds(0, cols)]
        to_right = (h == 0) == LONG[j]
        return pltpu.make_async_remote_copy(
            src_ref=stage.at[j % 2, c, pl.ds(h * half, half)], dst_ref=dst,
            send_sem=rs_send.at[h, j, c], recv_sem=rs_recv.at[h, j, c],
            device_id=right if to_right else left, device_id_type=MESH)

    def landed(j, c, h, at):
        if j == 0:
            return first[h, c, :, pl.ds(at, TILE)].astype(F32)
        row = pl.multiple_of(((j - 1) * CHUNKS + c) * half, half)
        return (wgv, wuv)[h][pl.ds(row, half), pl.ds(at, TILE)].astype(F32)

    def term(k, c, at):
        return jnp.dot(hid[k], wdv[:, pl.ds(pl.multiple_of(c * cols + at, TILE), TILE)], preferred_element_type=F32)

    def sum_step(j):
        @pl.loop(0, CHUNKS)
        def _(c):
            if FROM[j] is not None:
                for h in (0, 1):
                    rs(FROM[j], c, h).wait_recv()
            if j >= 2:
                for h in (0, 1):
                    rs(j - 2, c, h).wait_send()

            @pl.loop(0, cols // TILE)
            def _(t):
                at = pl.multiple_of(t * TILE, TILE)
                acc = term(PAIR[j], c, at)
                for h in (0, 1):
                    part = acc[h * half:(h + 1) * half]
                    if FROM[j] is not None:
                        part = part + landed(FROM[j], c, h, at)
                    stage[j % 2, c, pl.ds(h * half, half), pl.ds(at, TILE)] = part.astype(BF16)

            for h in (0, 1):
                rs(j, c, h).start()

    own = pltpu.make_async_copy(x, xv, x_sem)
    own.start()
    own.wait()
    wcopies[0].wait()
    wcopies[1].wait()
    hidden_of(0)
    pl.loop(1, 7)(gather_step)
    wcopies[2].wait()
    sum_step(0)
    ag(7, 1).wait_recv()
    for i in range(3):
        last(i).wait_recv()
    load_hidden(7)
    pl.semaphore_signal(free.at[1], inc=1, device_id=right, device_id_type=MESH)
    pl.semaphore_signal(free.at[0], inc=1, device_id=left, device_id_type=MESH)
    pl.semaphore_wait(free.at[0], 1)
    pl.semaphore_wait(free.at[1], 1)
    for j in range(1, 7):
        sum_step(j)

    @pl.loop(0, CHUNKS)
    def _(c):
        for h in (0, 1):
            rs(4, c, h).wait_recv()

        @pl.loop(0, cols // TILE)
        def _(t):
            at = pl.multiple_of(t * TILE, TILE)
            acc = term(0, c, at)
            for h in (0, 1):
                total[pl.ds(h * half, half), pl.ds(at, TILE)] = acc[h * half:(h + 1) * half] + landed(4, c, h, at)

        for h in (0, 1):
            rs(6, c, h).wait_recv()

        @pl.loop(0, cols // TILE)
        def _(t):
            at = pl.multiple_of(t * TILE, TILE)
            for h in (0, 1):
                rows = pl.ds(h * half, half)
                y[rows, pl.ds(pl.multiple_of(c * cols + at, TILE), TILE)] = (
                    total[rows, pl.ds(at, TILE)] + landed(6, c, h, at)).astype(BF16)

    @pl.loop(0, CHUNKS)
    def _(c):
        for h in (0, 1):
            rs(5, c, h).wait_send()
            rs(6, c, h).wait_send()

    @pl.loop(1, 7)
    def _(k):
        for d in (0, 1):
            ag(k, d).wait_send()

    ag(7, 1).wait_send()
    for i in range(3):
        last(i).wait_send()


def solution(mesh):
    n = mesh.shape["tp"]

    def step(x, w_gate, w_up, w_down):
        rows, d = x.shape
        width = w_gate.shape[1]
        half, cols = rows // 2, d // CHUNKS
        dma = pltpu.SemaphoreType.DMA
        y, _ = pl.pallas_call(
            functools.partial(kernel, n),
            out_shape=(pltpu.VMEM((rows, d), BF16), jax.ShapeDtypeStruct((n - 1, rows, d), BF16)),
            in_specs=[pl.BlockSpec(memory_space=pl.ANY)] * 4,
            out_specs=(pl.BlockSpec(memory_space=pltpu.VMEM), pl.BlockSpec(memory_space=pl.ANY)),
            scratch_shapes=[
                pltpu.VMEM((d, width), BF16),
                pltpu.VMEM((d, width), BF16),
                pltpu.VMEM((width, d), BF16),
                pltpu.VMEM((n, rows, width), BF16),
                pltpu.VMEM((rows, d), BF16),
                pltpu.VMEM((2, CHUNKS, rows, cols), BF16),
                pltpu.VMEM((2, CHUNKS, half, cols), BF16),
                pltpu.VMEM((rows, cols), F32),
                dma((3,)),
                dma,
                dma((2, n - 1)),
                dma((2, n - 1)),
                dma((3,)),
                dma((3,)),
                dma((2, 7, CHUNKS)),
                dma((2, 7, CHUNKS)),
                pltpu.SemaphoreType.REGULAR((2,)),
            ],
            compiler_params=pltpu.CompilerParams(
                collective_id=0, has_side_effects=True, vmem_limit_bytes=67043328 - 2 * rows * d),
            cost_estimate=pl.CostEstimate(
                flops=6 * n * rows * d * width, bytes_accessed=6 * d * width + 4 * n * rows * d, transcendentals=n * rows * width),
        )(x, w_gate, w_up, w_down)
        return y

    return jax.shard_map(
        step,
        mesh=mesh,
        in_specs=(P(("dp", "tp"), None), P(None, "tp"), P(None, "tp"), P("tp", None)),
        out_specs=P(("dp", "tp"), None),
        check_vma=False,
    )
```
